1024 devices in a mesh: gx: 4 (over x_hi), gy: 16 (over x_lo, z), gz: 16 (over y, core).
Axes of the slice: x: 8 (x_hi: 4, x_lo: 2; x = x_hi * 2 + x_lo), y: 8, z: 8, core: 2. Of those that a mesh axis runs over, the one named last changes fastest.
Arguments:
- offsets: float32 [3, 8, 64, 16, 256], P(None, 'gx', 'gy', 'gz'), may hold values from 0 to 1
- velocity: float32 [3, 8, 64, 16, 256], P(None, 'gx', 'gy', 'gz'), may hold values from -6 to 6
- mass: float32 [8, 64, 16, 256], P('gx', 'gy', 'gz'), may hold values from 0.004 to 0.04
- counts: int32 [8, 64, 16], P('gx', 'gy', 'gz'), may hold values from 64 to 256
Outputs:
- new_offsets: float32 [3, 8, 64, 16, 256], P(None, 'gx', 'gy', 'gz')
- new_velocity: float32 [3, 8, 64, 16, 256], P(None, 'gx', 'gy', 'gz')
The draws below stay inside these ranges and needn't reach their ends.
Inputs may be any that keep to these rules, and one draw needn't show every extreme that they name: `counts`: slots at or past a leaf's count are padding; their masses and positions carry no meaning as sources.
All inputs are finite; a program needn't handle non-finite values.
Results may differ from the reference program's by a relative error of at most 0.0001.
Values sent between devices are 32-bit elements; how exact they have to be, the bound alone decides.
A program may use at most 32 MiB of HBM per device.

```python
import math
import jax
import jax.numpy as jnp
import numpy as np
from jax import lax

SLOTS = 256
SUBSTEPS = 2
LEAVES_X = 8
LEAVES_Y = 64
LEAVES_Z = 16


def set_ends(result, own_key, smallest, largest):
    longest = result.shape.index(max(result.shape))
    spots = []
    for shift in (0, 1):
        where = [jax.random.randint(jax.random.fold_in(own_key, axis), (), 0, length) for axis, length in enumerate(result.shape)]
        where[longest] = (where[longest] + shift) % result.shape[longest]
        spots.append(tuple(where))
    return result.at[spots[0]].set(smallest).at[spots[1]].set(largest)


def level_of(rng, extent, pieces, least, high):
    gain, own = 1.0, jax.random.fold_in(rng, 6)
    for axis_at, parts in pieces:
        heights = jnp.exp(jax.random.uniform(jax.random.fold_in(own, axis_at), (parts,), jnp.float32, least / len(pieces), high / len(pieces)))
        gain = gain * jnp.repeat(heights, extent[axis_at] // parts).reshape([-1 if axis == axis_at else 1 for axis in range(len(extent))])
    return gain


def noise(key, shape, spread, bound, cuts=(), held_as=jnp.bfloat16):
    gain = level_of(key, shape, cuts, -0.22, 0.18) if cuts else 1.0
    values = jax.random.normal(key, shape, jnp.float32) * spread * gain
    return jnp.minimum(jnp.maximum(values, -bound), bound).astype(held_as)


def setup_inputs(seed: int = 0) -> dict:
    streams_of = jax.random.split(jax.random.key(seed), 5)
    offsets = jnp.clip(1.0 * jax.random.uniform(streams_of[0], (3, LEAVES_X, LEAVES_Y, LEAVES_Z, SLOTS), jnp.float32) ** level_of(streams_of[0], (3, LEAVES_X, LEAVES_Y, LEAVES_Z, SLOTS), ((1, 4), (2, 16), (3, 16)), -0.2, 0.2), 0.0, 1.0)
    velocity = noise(streams_of[1], (3, LEAVES_X, LEAVES_Y, LEAVES_Z, SLOTS), 1.0, 6.0, ((1, 4), (2, 16), (3, 16)), jnp.float32)
    mass = jnp.clip(jnp.exp(math.log(0.04) - 2.30258502 * jax.random.uniform(streams_of[2], (LEAVES_X, LEAVES_Y, LEAVES_Z, SLOTS), jnp.float32) ** level_of(streams_of[2], (LEAVES_X, LEAVES_Y, LEAVES_Z, SLOTS), ((0, 4), (1, 16), (2, 16)), -0.2, 0.2)), 0.004, 0.04)
    counts = set_ends(jax.random.randint(streams_of[3], (LEAVES_X, LEAVES_Y, LEAVES_Z), SLOTS // 4, SLOTS + 1), jax.random.fold_in(streams_of[3], 1), SLOTS // 4, SLOTS).astype(jnp.int32)
    return dict(offsets=offsets, velocity=velocity, mass=mass, counts=counts)


def pair_tile(target, source, shift):
    dist = source[:3, ..., None, :] + shift.reshape((3,) + (1,) * (source.ndim)) - target[..., :, None]
    square = jnp.sum(dist * dist, axis=0)
    factor = (square + 0.01) ** (-1.5) * jnp.maximum(1.0 - square, 0.0) ** 2
    scaled = source[3][..., None, :] * factor
    return jnp.sum(scaled[None] * dist, axis=-1)


def accel(position, weight):
    source = jnp.concatenate([position, weight[None]], axis=0)
    table = jnp.array(np.array([[a, b, c] for a in (-1, 0, 1) for b in (-1, 0, 1) for c in (-1, 0, 1)], dtype=np.int32))

    def one_offset(total, offset):
        rolled = jnp.roll(source, (-offset[0], -offset[1], -offset[2]), axis=(1, 2, 3))
        shift = offset.astype(jnp.float32)
        tiles = lax.map(lambda pair: pair_tile(pair[0], pair[1], shift),
                        (jnp.moveaxis(position, 1, 0), jnp.moveaxis(rolled, 1, 0)))
        return total + jnp.moveaxis(tiles, 0, 1), None

    total, _ = lax.scan(one_offset, jnp.zeros_like(position), table)
    return total


def reference(offsets, velocity, mass, counts):
    slot = jnp.arange(mass.shape[-1], dtype=jnp.int32)
    weight = jnp.where(slot < counts[..., None], mass, jnp.float32(0.0))
    position, speed = offsets, velocity
    for step in range(SUBSTEPS):
        speed = speed + 0.1 * accel(position, weight)
        position = position + 0.1 * speed
    return position, speed
```

```python
import functools
import jax
import jax.numpy as jnp
from jax import lax
from jax.experimental import pallas as pl
from jax.experimental.pallas import tpu as pltpu
from jax.sharding import PartitionSpec as P

SUBSTEPS = 2

RUN = 40
U = 4
MOST = 10
FEAT = 4


def split3(x):
    h = x.astype(jnp.bfloat16).astype(jnp.float32)
    rest = x - h
    m = rest.astype(jnp.bfloat16).astype(jnp.float32)
    low = (rest - m).astype(jnp.bfloat16).astype(jnp.float32)
    return h, m, low


def force_kernel(dims, counts_ref, src_ref, vel_ref, pos_out, vel_out,
                 table, feat, coef, tgt, acc, stage_a, stage_b, bounds, items):
    nx, ny, nz = dims
    ex, ey, ez = nx + 2, ny + 2, nz + 2
    row = lax.broadcasted_iota(jnp.int32, (8, 128), 0)
    lane = lax.broadcasted_iota(jnp.int32, (8, 128), 1)
    comp = row % 4
    center = (nx / 2.0, ny / 2.0, nz / 2.0)

    def frame(x, y, z):
        shift = [c - m - 1.0 for c, m in zip((x, y, z), center)]
        return jnp.where(comp == 0, shift[0], jnp.where(comp == 1, shift[1], jnp.where(comp == 2, shift[2], 0.0)))

    table[...] = jnp.zeros_like(table)
    ends = []
    points = {}
    for x in range(ex):
        off = jnp.int32(x * RUN * 128)
        for y in range(ey):
            points[(x, y)] = off
            for z in range(ez):
                e = (x * ey + y) * ez + z
                tile = src_ref[e] + frame(x, y, z)
                s = off & 127
                base = lax.shift_right_logical(off, 7)
                low = pltpu.roll(tile, s, 1)
                high = pltpu.roll(low, 4, 0)
                keep = lane < s
                table[base] = jnp.where(keep, table[base], low)
                table[base + 1] = jnp.where(keep, low, high)
                table[base + 2] = jnp.where(keep, high, 0.0)
                off = off + counts_ref[e]
        points[(x, ey)] = off
        ends.append(off)

    n = jnp.int32(0)
    for x in range(nx):
        for y in range(ny):
            for r in range(3):
                start = points[(x + r, y)]
                end = points[(x + r, y + 3)]
                first = lax.shift_right_logical(start, 7)
                last = lax.shift_right_logical(end + 127, 7)
                chunks = lax.shift_right_logical(last - first + 1, 1)
                tag = ((x * ny + y) * 4 + r)
                bounds[0, tag] = start
                bounds[1, tag] = end
                for j in range(MOST):
                    items[n + j] = first + (2 * j + tag * 256)
                n = n + chunks
    for j in range(4 * U):
        items[n + j] = (nx * ny * 4 - 1) * 256
    bounds[0, nx * ny * 4 - 1] = 0
    bounds[1, nx * ny * 4 - 1] = 0

    def norm(v):
        sq = jnp.where(row < 3, v * v, 0.0)
        sq = sq + pltpu.roll(sq, 4, 0)
        sq = sq + pltpu.roll(sq, 2, 0)
        return sq + pltpu.roll(sq, 1, 0)

    zeros = jnp.zeros((8, 128), jnp.float32)

    def features(t):
        v = table[t]
        full = jnp.where(row < 3, v, jnp.where(row < 6, pltpu.roll(v * v, 3, 0), jnp.where(row == 6, 1.0, 0.0)))
        h, m, low = split3(full)
        feat[t] = jnp.concatenate([h, m, low, h, m, h], axis=0).astype(jnp.bfloat16)
        mass = jnp.broadcast_to(v[3:4], (8, 128))
        gh, gm, gl = split3(jnp.where(row < 3, v, 1.0) * mass)
        coef[t] = jnp.concatenate([gh, gm, gl, zeros], axis=0)

    for x in range(ex):
        first = x * RUN
        count = lax.shift_right_logical(ends[x] + 127, 7) - first + 1

        def group(k, c, first=first):
            for j in range(FEAT):
                features(first + FEAT * k + j)
            return c

        lax.fori_loop(0, (count + FEAT - 1) // FEAT, group, 0)

    for x in range(nx):
        for y in range(ny):
            e = ((x + 1) * ey + y + 1) * ez + 1
            tile = src_ref[e] + frame(x + 1, y + 1, 1)
            for half in range(2):
                v = tile if half == 0 else pltpu.roll(tile, 4, 0)
                full = jnp.where(row < 3, -2.0 * v, jnp.where(row < 6, 1.0, jnp.where(row == 6, norm(v) + 0.01, 0.0)))
                h, m, low = split3(full)
                stacked = jnp.concatenate([h, h, h, m, m, low], axis=0)
                tgt[x * ny + y, :, half * 128:(half + 1) * 128] = stacked.astype(jnp.bfloat16)
    acc[...] = jnp.zeros_like(acc)

    lane32 = lax.broadcasted_iota(jnp.int32, (32, 256), 1)

    def squares(k, u, stage):
        code = items[k]
        t = code & 255
        leaf = lax.shift_right_logical(code, 10)
        f = jnp.concatenate([feat[t], feat[t + 1]], axis=1)
        stage[u] = lax.dot_general(f, tgt[leaf], (((0,), (0,)), ((), ())), preferred_element_type=jnp.float32)

    def gather(k, u, stage):
        code = items[k]
        t = code & 255
        tag = lax.shift_right_logical(code, 8)
        leaf = lax.shift_right_logical(code, 10)
        lo = bounds[0, tag] - t * 128
        hi = bounds[1, tag] - t * 128
        q = stage[u]
        r = lax.rsqrt(q)
        a = r * jnp.maximum(1.01 - q, 0.0)
        w = a * a * r
        whi = w.astype(jnp.bfloat16)
        wlo = (w - whi.astype(jnp.float32)).astype(jnp.bfloat16)
        cc = jnp.concatenate([coef[t], coef[t + 1]], axis=1)
        cc = jnp.where((lane32 >= lo) & (lane32 < hi), cc, 0.0).astype(jnp.bfloat16)
        out = jnp.dot(cc, whi, preferred_element_type=jnp.float32)
        out = out + jnp.dot(cc, wlo, preferred_element_type=jnp.float32)
        acc[leaf] = acc[leaf] + out

    for u in range(U):
        squares(u, u, stage_a)

    def step(i, c):
        k = i * (2 * U)
        for u in range(U):
            squares(k + U + u, u, stage_b)
            gather(k + u, u, stage_a)
        for u in range(U):
            squares(k + 2 * U + u, u, stage_a)
            gather(k + U + u, u, stage_b)
        return c

    lax.fori_loop(0, (n + 2 * U - 1) // (2 * U), step, 0)

    for x in range(nx):
        for y in range(ny):
            leaf = x * ny + y
            e = ((x + 1) * ey + y + 1) * ez + 1
            total = acc[leaf]
            total = total[0:8] + total[8:16] + total[16:24]
            tile = src_ref[e]
            where = tile + frame(x + 1, y + 1, 1)
            parts = []
            for half in range(2):
                v = where if half == 0 else pltpu.roll(where, 4, 0)
                part = total[:, half * 128:(half + 1) * 128]
                parts.append(part - v * jnp.broadcast_to(part[3:4], (8, 128)))
            kick = jnp.where(row < 4, parts[0], pltpu.roll(parts[1], 4, 0))
            kick = jnp.where(comp < 3, kick, 0.0)
            speed = vel_ref[leaf] + 0.1 * kick
            vel_out[leaf] = speed
            pos_out[leaf] = tile + 0.1 * speed


def forces(counts, source, velocity, dims):
    nx, ny, nz = dims
    ex, ey, ez = nx + 2, ny + 2, nz + 2
    leaves = nx * ny
    tiles = ex * RUN
    shape = jax.ShapeDtypeStruct((leaves, 8, 128), jnp.float32)
    return pl.pallas_call(
        functools.partial(force_kernel, dims),
        out_shape=(shape, shape),
        in_specs=[pl.BlockSpec(memory_space=pltpu.SMEM), pl.BlockSpec(memory_space=pltpu.VMEM),
                  pl.BlockSpec(memory_space=pltpu.VMEM)],
        out_specs=(pl.BlockSpec(memory_space=pltpu.VMEM), pl.BlockSpec(memory_space=pltpu.VMEM)),
        scratch_shapes=[
            pltpu.VMEM((tiles, 8, 128), jnp.float32),
            pltpu.VMEM((tiles, 48, 128), jnp.bfloat16),
            pltpu.VMEM((tiles, 32, 128), jnp.float32),
            pltpu.VMEM((leaves, 48, 256), jnp.bfloat16),
            pltpu.VMEM((leaves, 32, 256), jnp.float32),
            pltpu.VMEM((U, 256, 256), jnp.float32),
            pltpu.VMEM((U, 256, 256), jnp.float32),
            pltpu.SMEM((2, leaves * 4), jnp.int32),
            pltpu.SMEM((leaves * 3 * MOST + 4 * U,), jnp.int32),
        ],
        name="forces",
    )(counts, source, velocity)

OFFSETS = sorted(
    [(a, b, c) for a in (-1, 0, 1) for b in (-1, 0, 1) for c in (-1, 0, 1) if (a, b, c) != (0, 0, 0)],
    key=lambda o: (-abs(o[0]), -abs(o[1]), -abs(o[2]), o),
)
AXES = ("gx", "gy", "gz")


def exchange_kernel(sizes, dims, own_ref, ext_ref, local_sem, send_sem, recv_sem):
    me = [lax.axis_index(axis) for axis in AXES]
    peers = [tuple(lax.rem(m + o + n, n) for m, o, n in zip(me, offset, sizes)) for offset in OFFSETS]
    barrier = pltpu.get_barrier_semaphore()
    for peer in peers:
        pl.semaphore_signal(barrier, inc=1, device_id=peer, device_id_type=pl.DeviceIdType.MESH)
    middle = pltpu.make_async_copy(own_ref, ext_ref.at[tuple(pl.ds(1, d) for d in dims)], local_sem)
    middle.start()
    pl.semaphore_wait(barrier, len(peers))
    copies = []
    for k, (offset, peer) in enumerate(zip(OFFSETS, peers)):
        source = tuple(pl.ds(0, d) if o == 0 else pl.ds(d - 1 if o > 0 else 0, 1) for o, d in zip(offset, dims))
        target = tuple(pl.ds(1, d) if o == 0 else pl.ds(0 if o > 0 else d + 1, 1) for o, d in zip(offset, dims))
        copy = pltpu.make_async_remote_copy(
            src_ref=own_ref.at[source],
            dst_ref=ext_ref.at[target],
            send_sem=send_sem.at[k],
            recv_sem=recv_sem.at[k],
            device_id=peer,
            device_id_type=pl.DeviceIdType.MESH,
        )
        copy.start()
        copies.append(copy)
    middle.wait()
    for copy in copies:
        copy.wait()


def exchange(own, sizes, collective_id):
    dims = own.shape[:3]
    count = len(OFFSETS)
    return pl.pallas_call(
        functools.partial(exchange_kernel, sizes, dims),
        out_shape=jax.ShapeDtypeStruct(tuple(d + 2 for d in dims) + (8, 128), jnp.float32),
        in_specs=[pl.BlockSpec(memory_space=pltpu.VMEM)],
        out_specs=pl.BlockSpec(memory_space=pltpu.VMEM),
        scratch_shapes=[
            pltpu.SemaphoreType.DMA,
            pltpu.SemaphoreType.DMA((count,)),
            pltpu.SemaphoreType.DMA((count,)),
        ],
        compiler_params=pltpu.CompilerParams(collective_id=collective_id, has_side_effects=True),
        name="exchange",
    )(own)


def pack(fields):
    comps, nx, ny, nz, slots = fields.shape
    split = fields.reshape(comps, nx, ny, nz, 2, slots // 2)
    return jnp.transpose(split, (1, 2, 3, 4, 0, 5)).reshape(nx, ny, nz, 8, 128)


def unpack(tiles, dims):
    nx, ny, nz = dims
    split = tiles.reshape(nx, ny, nz, 2, 4, 128)[..., :3, :]
    return jnp.transpose(split, (4, 0, 1, 2, 3, 5)).reshape(3, nx, ny, nz, 256)


def shards(sizes, offsets, velocity, mass, counts):
    dims = mass.shape[:3]
    nx, ny, nz = dims
    slot = jnp.arange(mass.shape[-1], dtype=jnp.int32)
    weight = jnp.where(slot < counts[..., None], mass, jnp.float32(0.0))
    position = pack(jnp.concatenate([offsets, weight[None]], axis=0))
    speed = pack(jnp.concatenate([velocity, jnp.zeros_like(weight)[None]], axis=0))
    speed = speed.reshape(nx * ny * nz, 8, 128)
    live = None
    for _ in range(SUBSTEPS):
        source = exchange(position, sizes, 1).reshape(-1, 8, 128)
        if live is None:
            masses = jnp.concatenate([source[:, 3], source[:, 7]], axis=1)
            live = jnp.sum((masses > 0).astype(jnp.int32), axis=1)
        position, speed = forces(live, source, speed, dims)
        position = position.reshape(nx, ny, nz, 8, 128)
    return unpack(position, dims), unpack(speed, dims)


def solution(mesh):
    vector = P(None, "gx", "gy", "gz", None)
    return jax.shard_map(
        functools.partial(shards, tuple(mesh.shape[axis] for axis in AXES)),
        mesh=mesh,
        in_specs=(vector, vector, P("gx", "gy", "gz", None), P("gx", "gy", "gz")),
        out_specs=(vector, vector),
        check_vma=False,
    )
```

```python
import functools
import itertools

import jax
import jax.numpy as jnp
from jax import lax
from jax.experimental import pallas as pl
from jax.experimental.pallas import tpu as pltpu
from jax.sharding import PartitionSpec as P

SUBSTEPS = 2
AXES = ("gx", "gy", "gz")
MESH = pl.DeviceIdType.MESH
OFFSETS = sorted(
    [o for o in itertools.product((-1, 0, 1), repeat=3) if any(o)],
    key=lambda o: (-abs(o[2]) if o[:2] == (0, 0) else 0, -sum(abs(a) for a in o), o),
)
NX, NY, NZ = 2, 4, 1
U = 4


def split3(x):
    h = x.astype(jnp.bfloat16).astype(jnp.float32)
    rest = x - h
    m = rest.astype(jnp.bfloat16).astype(jnp.float32)
    return h, m, rest - m


def kernel(sizes, counts_ref, off_ref, mass_ref, vel_ref, pos_out, vel_out,
           ext, frames, speed, feat, coef, tgt, acc, stage_a, stage_b, send_sem, recv_sem):
    me = [lax.axis_index(axis) for axis in AXES]
    dims = (NX, NY, NZ)
    row = lax.broadcasted_iota(jnp.int32, (8, 128), 0)
    comp = row % 4
    lane = lax.broadcasted_iota(jnp.int32, (1, 128), 1)
    center = (slice(1, NX + 1), slice(1, NY + 1), slice(1, NZ + 1))

    def peer(offset):
        return tuple(lax.rem(m + o + n, n) for m, o, n in zip(me, offset, sizes))

    barrier = pltpu.get_barrier_semaphore()
    for offset in OFFSETS:
        pl.semaphore_signal(barrier, inc=1, device_id=peer(offset), device_id_type=MESH)

    def copies(step):
        out = {}
        for k, offset in enumerate(OFFSETS):
            source = tuple(pl.ds(d if o > 0 else 1, 1) if o else pl.ds(1, d) for o, d in zip(offset, dims))
            target = tuple(pl.ds(0 if o > 0 else d + 1, 1) if o else pl.ds(1, d) for o, d in zip(offset, dims))
            out[offset] = pltpu.make_async_remote_copy(
                src_ref=ext.at[(step,) + source],
                dst_ref=ext.at[(step,) + target],
                send_sem=send_sem.at[step, k],
                recv_sem=recv_sem.at[step, k],
                device_id=peer(offset),
                device_id_type=MESH,
            )
        return out

    for leaf in range(NX * NY):
        x, y = leaf // NY, leaf % NY
        for half in range(2):
            for c in range(3):
                r = c * 16 + leaf * 2 + half
                ext[0, x + 1, y + 1, 1, half * 4 + c:half * 4 + c + 1, :] = off_ref[r:r + 1, :]
                speed[leaf, half * 4 + c:half * 4 + c + 1, :] = vel_ref[r:r + 1, :]
            live = jnp.where(lane < counts_ref[leaf] - 128 * half, mass_ref[leaf * 2 + half:leaf * 2 + half + 1, :], 0.0)
            ext[0, x + 1, y + 1, 1, half * 4 + 3:half * 4 + 4, :] = live
            speed[leaf, half * 4 + 3:half * 4 + 4, :] = jnp.zeros((1, 128), jnp.float32)
    unit = [jnp.where(comp == c, 1.0, 0.0) for c in range(3)]
    for x in range(NX + 2):
        for y in range(NY + 2):
            for z in range(NZ + 2):
                shift = unit[0] * (x - NX / 2 - 1) + unit[1] * (y - NY / 2 - 1) + unit[2] * (z - NZ / 2 - 1)
                frames[x, y, z] = shift

    def spread(step, xs, ys, zs):
        lead = tuple(s.stop - s.start for s in (xs, ys, zs))
        n = lead[0] * lead[1] * lead[2]
        tile = (ext[step, xs, ys, zs] + frames[xs, ys, zs]).reshape(n, 8, 128)
        rows = lax.broadcasted_iota(jnp.int32, (n, 8, 128), 1)
        for half in range(2):
            v = tile if half == 0 else pltpu.roll(tile, 4, 1)
            full = jnp.where(rows < 3, v, jnp.where(rows < 6, pltpu.roll(v * v, 3, 1), jnp.where(rows == 6, 1.0, 0.0)))
            h, m, low = split3(full)
            f = jnp.concatenate([h, m, low, h, m, h], axis=1).astype(jnp.bfloat16)
            cols = slice(half * 128, half * 128 + 128)
            feat[xs, ys, zs, :, cols] = f.reshape(lead + (48, 128))
            g = jnp.where(rows < 3, v, 1.0) * jnp.broadcast_to(v[:, 3:4, :], (n, 8, 128))
            h, m, low = split3(g)
            f = jnp.concatenate([h, m, low, jnp.zeros_like(h)], axis=1).astype(jnp.bfloat16)
            coef[xs, ys, zs, :, cols] = f.reshape(lead + (32, 128))

    def aim(step):
        n = NX * NY
        tile = (ext[(step,) + center] + frames[center]).reshape(n, 8, 128)
        rows = lax.broadcasted_iota(jnp.int32, (n, 8, 128), 1)
        for half in range(2):
            v = tile if half == 0 else pltpu.roll(tile, 4, 1)
            sq = jnp.where(rows < 3, v * v, 0.0)
            sq = sq + pltpu.roll(sq, 4, 1)
            sq = sq + pltpu.roll(sq, 2, 1)
            sq = sq + pltpu.roll(sq, 1, 1)
            full = jnp.where(rows < 3, -2.0 * v, jnp.where(rows < 6, 1.0, jnp.where(rows == 6, sq + 0.01, 0.0)))
            h, m, low = split3(full)
            f = jnp.concatenate([h, h, h, m, m, low], axis=1).astype(jnp.bfloat16)
            tgt[:, :, half * 128:half * 128 + 128] = f

    def squares(place, stage, u):
        x, y, z, leaf = place
        stage[u] = lax.dot_general(
            feat[x, y, z], tgt[leaf], (((0,), (0,)), ((), ())), preferred_element_type=jnp.float32)

    def gather(place, stage, u):
        x, y, z, leaf = place
        q = stage[u]
        r = lax.rsqrt(q)
        a = r * jnp.maximum(1.01 - q, 0.0)
        w = a * a * r
        whi = w.astype(jnp.bfloat16)
        wlo = (w - whi.astype(jnp.float32)).astype(jnp.bfloat16)
        cc = coef[x, y, z]
        out = jnp.dot(cc, whi, preferred_element_type=jnp.float32)
        acc[leaf] += out + jnp.dot(cc, wlo, preferred_element_type=jnp.float32)

    def pairs(place, trips):
        for u in range(U):
            squares(place(0, u), stage_a, u)

        def trip(i, carry):
            later = jnp.minimum(i + 1, trips - 1)
            for u in range(U):
                squares(place(i, U + u), stage_b, u)
                gather(place(i, u), stage_a, u)
            for u in range(U):
                squares(place(later, u), stage_a, u)
                gather(place(i, U + u), stage_b, u)
            return carry

        lax.fori_loop(0, trips, trip, 0)

    def brick(layer):
        def place(i, j):
            p = i * 2 + j // 4
            ty = lax.div(jnp.int32(p + 1), jnp.int32(3))
            tx, sx = (j // 2) % 2, j % 2
            return sx + 1, p - 2 * ty + 1, layer, tx * NY + ty
        return place

    def sides(i, j):
        z = lax.div(jnp.int32(i), jnp.int32(3))
        b = i - 3 * z
        ty, side = j // 2, j % 2
        return 3 * side, ty + b, z, side * NY + ty

    def fronts(i, j):
        tx, sx, side = j // 4, (j // 2) % 2, j % 2
        return sx + 1, 5 * side, i, tx * NY + 3 * side

    def finish(step):
        for leaf in range(NX * NY):
            x, y = leaf // NY, leaf % NY
            total = acc[leaf]
            total = total[0:8] + total[8:16] + total[16:24]
            tile = ext[step, x + 1, y + 1, 1]
            where = tile + frames[x + 1, y + 1, 1]
            parts = []
            for half in range(2):
                v = where if half == 0 else pltpu.roll(where, 4, 0)
                part = total[:, half * 128:half * 128 + 128]
                parts.append(part - v * jnp.broadcast_to(part[3:4], (8, 128)))
            kick = jnp.where(row < 4, parts[0], pltpu.roll(parts[1], 4, 0))
            fresh = speed[leaf] + 0.1 * jnp.where(comp < 3, kick, 0.0)
            moved = tile + 0.1 * fresh
            if step + 1 < SUBSTEPS:
                speed[leaf] = fresh
                ext[step + 1, x + 1, y + 1, 1] = moved
            else:
                for half in range(2):
                    for c in range(3):
                        r, k = c * 16 + leaf * 2 + half, half * 4 + c
                        pos_out[r:r + 1, :] = moved[k:k + 1]
                        vel_out[r:r + 1, :] = fresh[k:k + 1]

    low, high = (0, 0, -1), (0, 0, 1)
    for step in range(SUBSTEPS):
        moves = copies(step)
        acc[...] = jnp.zeros_like(acc)
        aim(step)
        spread(step, *center)
        if step == 0:
            pairs(brick(1), 5)
            pl.semaphore_wait(barrier, len(OFFSETS))
        for offset in OFFSETS:
            moves[offset].start()
        if step > 0:
            pairs(brick(1), 5)
        moves[low].wait_recv()
        moves[high].wait_recv()
        spread(step, center[0], center[1], slice(0, 1))
        spread(step, center[0], center[1], slice(2, 3))
        pairs(brick(0), 5)
        pairs(brick(2), 5)
        for offset in OFFSETS:
            if offset not in (low, high):
                moves[offset].wait_recv()
        spread(step, slice(0, 1), slice(0, NY + 2), slice(0, 3))
        spread(step, slice(3, 4), slice(0, NY + 2), slice(0, 3))
        spread(step, center[0], slice(0, 1), slice(0, 3))
        spread(step, center[0], slice(NY + 1, NY + 2), slice(0, 3))
        pairs(sides, 9)
        pairs(fronts, 3)
        finish(step)
        for offset in OFFSETS:
            moves[offset].wait_send()


def shards(sizes, offsets, velocity, mass, counts):
    leaves = NX * NY
    shell = (NX + 2, NY + 2, NZ + 2)
    flat = jax.ShapeDtypeStruct((6 * leaves, 128), jnp.float32)
    vmem = pl.BlockSpec(memory_space=pltpu.VMEM)
    position, speed = pl.pallas_call(
        functools.partial(kernel, sizes),
        out_shape=(flat, flat),
        in_specs=[pl.BlockSpec(memory_space=pltpu.SMEM), vmem, vmem, vmem],
        out_specs=(vmem, vmem),
        scratch_shapes=[
            pltpu.VMEM((SUBSTEPS,) + shell + (8, 128), jnp.float32),
            pltpu.VMEM(shell + (8, 128), jnp.float32),
            pltpu.VMEM((leaves, 8, 128), jnp.float32),
            pltpu.VMEM(shell + (48, 256), jnp.bfloat16),
            pltpu.VMEM(shell + (32, 256), jnp.bfloat16),
            pltpu.VMEM((leaves, 48, 256), jnp.bfloat16),
            pltpu.VMEM((leaves, 32, 256), jnp.float32),
            pltpu.VMEM((U, 256, 256), jnp.float32),
            pltpu.VMEM((U, 256, 256), jnp.float32),
            pltpu.SemaphoreType.DMA((SUBSTEPS, len(OFFSETS))),
            pltpu.SemaphoreType.DMA((SUBSTEPS, len(OFFSETS))),
        ],
        compiler_params=pltpu.CompilerParams(
            collective_id=1, has_side_effects=True),
        name="substeps",
    )(counts.reshape(leaves), offsets.reshape(6 * leaves, 128), mass.reshape(2 * leaves, 128),
      velocity.reshape(6 * leaves, 128))
    return position.reshape(offsets.shape), speed.reshape(velocity.shape)


def solution(mesh):
    vector = P(None, "gx", "gy", "gz", None)
    return jax.shard_map(
        functools.partial(shards, tuple(mesh.shape[axis] for axis in AXES)),
        mesh=mesh,
        in_specs=(vector, vector, P("gx", "gy", "gz", None), P("gx", "gy", "gz")),
        out_specs=(vector, vector),
        check_vma=False,
    )
```
